32 devices in a mesh: blk: 16 (over z, y, core), rhs: 2 (over x).
Axes of the slice: x: 2, y: 2, z: 4, core: 2. Of those that a mesh axis runs over, the one named last changes fastest.
Arguments:
- signal: bfloat16 [131072, 256], P('blk', 'rhs'), may hold values from -6 to 6
- col_factor: bfloat16 [96, 131072], P(None, 'blk'), may hold values from -0.5 to 0.5
- row_factor: bfloat16 [96, 131072], P(None, 'blk'), may hold values from -0.625 to 0.625
- level_factor: bfloat16 [4, 16, 2, 64, 48, 192], P(None, 'blk', None, 'rhs'), may hold values from -0.4375 to 0.4375
- col_leaf_sizes: int32 [16, 128], P('blk'), may hold values from 1 to 128, 8192 in all within a row
- row_leaf_sizes: int32 [16, 128], P('blk'), may hold values from 1 to 128, 8192 in all within a row
- level_order: int32 [4, 16, 128], P(None, 'blk'), may hold values from 0 to 127, each once within a row
Outputs:
- result: bfloat16 [131072, 256], P('blk', 'rhs')
The draws below stay inside these ranges and needn't reach their ends.
Inputs may be any that keep to these rules, and one draw needn't show every extreme that they name: `col_leaf_sizes`: row d lists in order the sizes of the 128 column leaves that cover unknowns d * 8192 to (d + 1) * 8192 - 1; each row sums to 8192 and its largest entry is 128. `row_leaf_sizes`: row d lists in order the sizes of the 128 row leaves that cover unknowns d * 8192 to (d + 1) * 8192 - 1; each row sums to 8192 and its largest entry is 128. Every level_order[l, d, :] is a permutation of 0 to 127.
All inputs are finite; a program needn't handle non-finite values.
Results may differ from the reference program's by a relative error of at most 0.0076.
Values may be sent and summed in bfloat16 or wider, within the bound.
A program may use at most 128 MiB of HBM per device.

```python
import math
import jax
import jax.numpy as jnp
import numpy as np
from jax import lax

K = 48
P_DEV = 8192
LEAVES_DEV = 128
LEAFMAX = 128
LEVELS = 4
COLS_DEV = 64
GROUPS = 16
R = 128
N = 131072
PEER_BLOCKS = 8


def block_levels(own_key, shape, split, least, high):
    def one(axis_at, parts):
        steps = jax.random.uniform(jax.random.fold_in(jax.random.fold_in(own_key, 6), axis_at), (parts,), jnp.float32, least / len(split), high / len(split))
        return jnp.repeat(jnp.exp(steps), shape[axis_at] // parts).reshape((-1,) + (1,) * (len(shape) - axis_at - 1))

    level = one(*split[0])
    for cut in split[1:]:
        level = level * one(*cut)
    return level


def length_profile(count, total, bound, slope):
    loads = [(1 << 20) // math.isqrt(standing ** slope) + 1 for standing in range(2, count + 1)]
    rest, holding = total - bound - (count - 1), [1] * (count - 1)
    while rest > 0:
        movable = [i for i in range(count - 1) if holding[i] < bound]
        whole, budget = sum([loads[i] for i in movable]), rest
        for i in movable:
            more = min(bound - holding[i], max(1, budget * loads[i] // whole), rest)
            holding[i] = holding[i] + more
            rest = rest - more
    return np.array([bound] + holding)


def uneven_parts(stream_key, number_of, total, bound, slope):
    if number_of == 2:
        one = jax.random.randint(stream_key, (), max(1, total - bound), min(bound, total - 1) + 1)
        return jnp.stack([one, total - one])
    tallies = jnp.asarray(length_profile(number_of, total, bound, slope), jnp.int32)
    twos = (number_of - 1) // 2
    giver, receiver = tallies[1:1 + 2 * twos:2], tallies[2:2 + 2 * twos:2]
    margin = jnp.minimum(giver - 1, bound - receiver)
    passed = jax.random.randint(jax.random.fold_in(stream_key, 1), (twos,), 0, 1 << 20) % (margin + 1)
    tallies = tallies.at[1:1 + 2 * twos:2].set(giver - passed).at[2:2 + 2 * twos:2].set(receiver + passed)
    return tallies[jax.random.permutation(jax.random.fold_in(stream_key, 2), number_of)]


def gaussian(key, extent, spread, limit, cuts=(), kind=jnp.bfloat16):
    loudness = block_levels(key, extent, cuts, -0.22, 0.18) if cuts else 1.0
    values = jax.random.normal(key, extent, jnp.float32) * spread * loudness
    return jnp.minimum(jnp.maximum(values, -limit), limit).astype(kind)


def setup_inputs(seed: int = 0) -> dict:
    seeds = jax.random.split(jax.random.key(seed), 8)
    return {
        "signal": gaussian(seeds[0], (N, 2 * R), 1.0, 6.0, ((0, 16), (1, 2))),
        "col_factor": gaussian(seeds[1], (2 * K, N), (2 * P_DEV // LEAVES_DEV) ** -0.5, 0.5, ((1, 16),)),
        "row_factor": gaussian(seeds[2], (2 * K, N), (2 * K) ** -0.5, 0.625, ((1, 16),)),
        "level_factor": gaussian(seeds[3], (LEVELS, GROUPS, 2, LEAVES_DEV // 2, K, 4 * K), (4 * K) ** -0.5, 0.4375, ((1, 16), (3, 2))),
        "col_leaf_sizes": jax.vmap(lambda own: uneven_parts(own, LEAVES_DEV, P_DEV, LEAFMAX, 1))(jax.random.split(seeds[4], GROUPS)).reshape((GROUPS, LEAVES_DEV)).astype(jnp.int32),
        "row_leaf_sizes": jax.vmap(lambda own: uneven_parts(own, LEAVES_DEV, P_DEV, LEAFMAX, 1))(jax.random.split(seeds[5], GROUPS)).reshape((GROUPS, LEAVES_DEV)).astype(jnp.int32),
        "level_order": jax.vmap(lambda own: jax.random.permutation(own, LEAVES_DEV))(jax.random.split(seeds[6], LEVELS * GROUPS)).reshape((LEVELS, GROUPS, LEAVES_DEV)).astype(jnp.int32),
    }


def turn_parts(values, groups):
    pieces = values.reshape(values.shape[:-1] + (groups, 2, values.shape[-1] // (2 * groups)))
    turned = jnp.stack([-pieces[..., 1, :], pieces[..., 0, :]], axis=-2)
    return turned.reshape(values.shape)


def leaf_windows(leaf_sizes):
    leaf_sizes = leaf_sizes.astype(jnp.int32)
    starts = (jnp.cumsum(leaf_sizes) - leaf_sizes).astype(jnp.int32)
    offsets = jnp.arange(LEAFMAX, dtype=jnp.int32)
    window_index = jnp.minimum(starts[:, None] + offsets[None, :], P_DEV - 1).astype(jnp.int32)
    inside = offsets[None, :] < leaf_sizes[:, None]
    return starts, window_index, inside


def leaf_coefficients(operands):
    points, factor, leaf_sizes = operands
    starts, window_index, inside = leaf_windows(leaf_sizes)
    flat_index = window_index.reshape(-1)
    gathered = jnp.take(points, flat_index, axis=0).reshape(LEAVES_DEV, LEAFMAX, points.shape[-1])
    weights = jnp.take(factor, flat_index, axis=1).reshape(2, K, LEAVES_DEV, LEAFMAX)
    weights = jnp.where(inside[None, None], weights, jnp.zeros_like(weights))
    paired = jnp.stack([gathered, turn_parts(gathered, R // COLS_DEV)])
    products = jnp.einsum("tkbi,tbic->bkc", weights.astype(jnp.float32), paired.astype(jnp.float32))
    return products.astype(jnp.bfloat16)


def mix_level(operands):
    arrived, weights = operands
    groups = R // COLS_DEV
    partner = jnp.roll(arrived, LEAVES_DEV // 2, axis=0)
    stacked = jnp.concatenate([arrived, turn_parts(arrived, groups), partner, turn_parts(partner, groups)], axis=1)
    products = jnp.einsum("bkm,bmc->bkc", weights.astype(jnp.float32), stacked.astype(jnp.float32))
    return products.astype(jnp.bfloat16)


def leaf_outputs(operands):
    coefficients, factor, leaf_sizes = operands
    starts, window_index, inside = leaf_windows(leaf_sizes)
    weights = jnp.take(factor, window_index.reshape(-1), axis=1).reshape(2, K, LEAVES_DEV, LEAFMAX)
    paired = jnp.stack([coefficients, turn_parts(coefficients, R // COLS_DEV)])
    leafwise = jnp.einsum("tkbi,tbkc->bic", weights.astype(jnp.float32), paired.astype(jnp.float32))
    points = jnp.arange(P_DEV, dtype=jnp.int32)
    covered = starts[None, :] <= points[:, None]
    leaf_index = (jnp.sum(covered.astype(jnp.int32), axis=1) - 1).astype(jnp.int32)
    leaf_start = jnp.max(jnp.where(covered, starts[None, :], jnp.zeros_like(starts)[None, :]), axis=1).astype(jnp.int32)
    flat_index = (leaf_index * LEAFMAX + points - leaf_start).astype(jnp.int32)
    return jnp.take(leafwise.reshape(-1, leafwise.shape[-1]), flat_index, axis=0).astype(jnp.bfloat16)


def reference(signal, col_factor, row_factor, level_factor, col_leaf_sizes, row_leaf_sizes, level_order):
    columns = signal.shape[-1]
    grouped = signal.reshape(GROUPS, P_DEV, columns)
    col_parts = col_factor.reshape(2 * K, GROUPS, P_DEV).transpose(1, 0, 2)
    coefficients = lax.map(leaf_coefficients, (grouped, col_parts, col_leaf_sizes))
    for layer_index in range(LEVELS):
        chosen = level_order[layer_index].astype(jnp.int32)[:, :, None, None]
        outgoing = jnp.take_along_axis(coefficients, chosen, axis=1)
        arrived = outgoing.reshape(GROUPS, GROUPS, PEER_BLOCKS, K, columns)
        arrived = arrived.transpose(1, 0, 2, 3, 4).reshape(GROUPS, LEAVES_DEV, K, columns)
        weights = level_factor[layer_index].reshape(GROUPS, LEAVES_DEV, K, 4 * K)
        coefficients = lax.map(mix_level, (arrived, weights))
    row_parts = row_factor.reshape(2 * K, GROUPS, P_DEV).transpose(1, 0, 2)
    outputs = lax.map(leaf_outputs, (coefficients, row_parts, row_leaf_sizes))
    return outputs.reshape(N, columns)
```

```python
import functools

import jax
import jax.numpy as jnp
from jax import lax
from jax.experimental import pallas as pl
from jax.experimental.pallas import tpu as pltpu
from jax.sharding import PartitionSpec as P

LANES = 128
ROWS = 16
CHUNKS = 2
AHEAD = 2
MESH = pl.DeviceIdType.MESH


def turn(values):
    half = values.shape[-1] // 2
    return jnp.concatenate([-values[:, half:], values[:, :half]], axis=1)


def levels_kernel(
    n, order, first_hbm, lf_hbm, coef,
    own, own_tail, far, far_tail, send, arr,
    load_sem, w_send, w_recv, a_send, a_recv,
):
    levels, _, depth, rank, width = own.shape
    blocks = coef.shape[0]
    per = blocks // n
    half = n // 2
    sources = n // 4
    step = depth // CHUNKS
    me = lax.axis_index("blk")
    col = lax.axis_index("rhs")

    def load(l):
        return pltpu.make_async_copy(lf_hbm.at[l], own.at[l], load_sem.at[l])

    load_coef = pltpu.make_async_copy(first_hbm, coef, load_sem.at[levels])
    load(0).start()
    load_coef.start()
    for l in range(1, levels):
        load(l).start()

    barrier = pltpu.get_barrier_semaphore()

    def greet(k, carry):
        peer = lax.rem(me + k, n)
        pl.semaphore_signal(barrier, inc=1, device_id=(peer, col), device_id_type=MESH)
        return carry

    lax.fori_loop(1, n, greet, 0)
    pl.semaphore_signal(barrier, inc=1, device_id=(me, 1 - col), device_id_type=MESH)

    def weight_copies(l, c):
        part = pl.ds(c * step, step)
        head = pltpu.make_async_remote_copy(
            src_ref=own.at[l, :, part, :, pl.ds(0, LANES)],
            dst_ref=far.at[l, :, part],
            send_sem=w_send.at[l, c, 0],
            recv_sem=w_recv.at[l, c, 0],
            device_id=(me, 1 - col),
            device_id_type=MESH,
        )
        tail = pltpu.make_async_remote_copy(
            src_ref=own_tail.at[l, part],
            dst_ref=far_tail.at[l, part],
            send_sem=w_send.at[l, c, 1],
            recv_sem=w_recv.at[l, c, 1],
            device_id=(me, 1 - col),
            device_id_type=MESH,
        )
        return head, tail

    def pack(l):
        def one(i, carry):
            own_tail[l, i] = jnp.concatenate(
                [own[l, 0, i, :, LANES:width], own[l, 1, i, :, LANES:width]], axis=1
            )
            return carry

        lax.fori_loop(0, depth, one, 0, unroll=4)

    def send_weights(l):
        for c in range(CHUNKS):
            for copy in weight_copies(l, c):
                copy.start()

    load(0).wait()
    pack(0)
    pl.semaphore_wait(barrier, n)
    send_weights(0)

    load_coef.wait()

    def block_copy(par, peer):
        return pltpu.make_async_remote_copy(
            src_ref=send.at[peer],
            dst_ref=arr.at[par, me],
            send_sem=a_send.at[peer],
            recv_sem=a_recv.at[par, me],
            device_id=(peer, col),
            device_id_type=MESH,
        )

    def arrival(par, source):
        return pltpu.make_async_remote_copy(
            src_ref=send.at[source],
            dst_ref=arr.at[par, source],
            send_sem=a_send.at[source],
            recv_sem=a_recv.at[par, source],
            device_id=(source, col),
            device_id_type=MESH,
        )

    blank = jnp.zeros((2 * LANES - width, LANES), jnp.bfloat16)

    def level(l, carry):
        par = lax.rem(l, 2)

        def choose(peer):
            for q in range(per):
                send[peer, q] = coef[order[l, peer * per + q]]

        def hand_out(k, inner):
            peer = lax.rem(me + k, n)
            choose(peer)
            block_copy(par, peer).start()
            return inner

        lax.fori_loop(1, n, hand_out, 0)
        choose(me)
        mine = pltpu.make_async_copy(send.at[me], arr.at[par, me], a_recv.at[par, me])
        mine.start()

        @pl.when(l == 0)
        def _():
            for later in range(1, levels):
                load(later).wait()
                pack(later)
            for later in range(1, AHEAD):
                send_weights(later)

        @pl.when(l + AHEAD < levels + 0)
        def _():
            send_weights(l + AHEAD)

        def combine(s, at, head, tail):
            arrival(par, s).wait_recv()
            arrival(par, s + half).wait_recv()
            for q in range(per):
                i = at * per + q
                x = arr[par, s, q]
                y = arr[par, s + half, q]
                jx = turn(x)
                jy = turn(y)
                rest = tail[l, i]
                upper = jnp.concatenate([head(0, i), rest], axis=1)
                lower = jnp.concatenate([head(1, i), rest], axis=1)
                cut = LANES - 2 * rank
                over = jnp.concatenate([x, jx, y, jy, blank], axis=0)
                under = jnp.concatenate([y, jy, x[:cut], blank, x[cut:], jx], axis=0)
                coef[s * per + q] = jnp.dot(
                    upper, over, preferred_element_type=jnp.float32
                ).astype(jnp.bfloat16)
                coef[(s + half) * per + q] = jnp.dot(
                    lower, under, preferred_element_type=jnp.float32
                ).astype(jnp.bfloat16)

        def near(k, inner):
            combine(col * sources + k, k, lambda h, i: own[l, h, i, :, :LANES], own_tail)
            return inner

        lax.fori_loop(0, sources, near, 0)

        def distant(k, inner):
            combine((1 - col) * sources + k, k, lambda h, i: far[l, h, i], far_tail)
            return inner

        for c in range(CHUNKS):
            for copy in weight_copies(l, c):
                copy.wait_recv()
            lax.fori_loop(c * (sources // CHUNKS), (c + 1) * (sources // CHUNKS), distant, 0)

        def sent(k, inner):
            block_copy(par, lax.rem(me + k, n)).wait_send()
            return inner

        lax.fori_loop(1, n, sent, 0)
        return carry

    lax.fori_loop(0, levels, level, 0)
    for l in range(levels):
        for c in range(CHUNKS):
            for copy in weight_copies(l, c):
                copy.wait_send()


def leaves_kernel(sizes, sig, cf, coef):
    blocks, rank, _ = coef.shape
    points = sig.shape[0]
    window = 2 * LANES
    lane = lax.broadcasted_iota(jnp.int32, (1, window), 1)

    def leaf(b, start):
        end = start + sizes[0, b]
        base = jnp.minimum(start // LANES * LANES, points - window)
        base = pl.multiple_of(base, LANES)
        inside = jnp.logical_and(lane >= start - base, lane < end - base)
        keep = jnp.where(inside, 1.0, 0.0).astype(jnp.bfloat16)
        weights = cf[:, pl.ds(base, window)] * keep
        sums = jnp.dot(weights, sig[pl.ds(base, window), :], preferred_element_type=jnp.float32)
        coef[b] = (sums[:rank] + turn(sums[rank:])).astype(jnp.bfloat16)
        return end

    lax.fori_loop(0, blocks, leaf, jnp.int32(0), unroll=4)


def rows_kernel(sizes, coef, rf, out_hbm, flipped, out, sem):
    blocks, rank, _ = coef.shape
    points = rf.shape[1]
    window = LANES + ROWS

    def flip(c, carry):
        base = pl.multiple_of(c * LANES, LANES)
        flipped[pl.ds(base, LANES), :] = rf[:, pl.ds(base, LANES)].T
        return carry

    lax.fori_loop(0, points // LANES, flip, 0, unroll=4)
    row = lax.broadcasted_iota(jnp.int32, (ROWS, LANES), 0)

    def leaf(b, start):
        base = pl.multiple_of(start // ROWS * ROWS, ROWS)
        values = coef[b]
        pair = jnp.concatenate([values, turn(values)], axis=0)
        sums = jnp.dot(flipped[pl.ds(base, window), :], pair, preferred_element_type=jnp.float32)
        before = out[pl.ds(base, ROWS), :].astype(jnp.float32)
        top = jnp.where(row < start - base, before, sums[:ROWS])
        out[pl.ds(base, ROWS), :] = top.astype(jnp.bfloat16)
        out[pl.ds(base + ROWS, LANES), :] = sums[ROWS:].astype(jnp.bfloat16)
        return start + sizes[0, b]

    lax.fori_loop(0, blocks, leaf, jnp.int32(0), unroll=4)
    copy = pltpu.make_async_copy(out.at[pl.ds(0, points)], out_hbm, sem)
    copy.start()
    copy.wait()


def local(
    n, signal, col_factor, row_factor, level_factor, col_leaf_sizes, row_leaf_sizes, level_order
):
    levels, _, halves, depth, rank, width = level_factor.shape
    blocks = col_leaf_sizes.shape[1]
    points, columns = signal.shape
    bf16 = jnp.bfloat16
    smem = pl.BlockSpec(memory_space=pltpu.SMEM)
    vmem = pl.BlockSpec(memory_space=pltpu.VMEM)
    anywhere = pl.BlockSpec(memory_space=pl.ANY)
    first = pl.pallas_call(
        leaves_kernel,
        out_shape=jax.ShapeDtypeStruct((blocks, row_factor.shape[0] // 2, columns), bf16),
        in_specs=[smem, vmem, vmem],
        out_specs=vmem,
        compiler_params=pltpu.CompilerParams(vmem_limit_bytes=32 << 20),
        name="leaves",
    )(col_leaf_sizes, signal, col_factor)
    factors = level_factor.reshape(levels, halves, depth, rank, width)
    coefficients = pl.pallas_call(
        functools.partial(levels_kernel, n),
        out_shape=jax.ShapeDtypeStruct((blocks, rank, columns), bf16),
        in_specs=[smem, anywhere, anywhere],
        out_specs=vmem,
        scratch_shapes=[
            pltpu.VMEM((levels, halves, depth, rank, width), bf16),
            pltpu.VMEM((levels, depth, rank, LANES), bf16),
            pltpu.VMEM((levels, halves, depth, rank, LANES), bf16),
            pltpu.VMEM((levels, depth, rank, LANES), bf16),
            pltpu.VMEM((n, blocks // n, rank, columns), bf16),
            pltpu.VMEM((2, n, blocks // n, rank, columns), bf16),
            pltpu.SemaphoreType.DMA((levels + 1,)),
            pltpu.SemaphoreType.DMA((levels, CHUNKS, 2)),
            pltpu.SemaphoreType.DMA((levels, CHUNKS, 2)),
            pltpu.SemaphoreType.DMA((n,)),
            pltpu.SemaphoreType.DMA((2, n)),
        ],
        compiler_params=pltpu.CompilerParams(
            collective_id=0, has_side_effects=True, vmem_limit_bytes=48 << 20
        ),
        name="levels",
    )(level_order.reshape(levels, blocks), first, factors)
    return pl.pallas_call(
        rows_kernel,
        out_shape=jax.ShapeDtypeStruct((points, columns), bf16),
        in_specs=[smem, vmem, vmem],
        out_specs=anywhere,
        scratch_shapes=[
            pltpu.VMEM((points + LANES + ROWS, 2 * rank), bf16),
            pltpu.VMEM((points + LANES + ROWS, columns), bf16),
            pltpu.SemaphoreType.DMA(()),
        ],
        compiler_params=pltpu.CompilerParams(vmem_limit_bytes=40 << 20),
        name="rows",
    )(row_leaf_sizes, coefficients, row_factor)


def solution(mesh):
    in_specs = (
        P("blk", "rhs"),
        P(None, "blk"),
        P(None, "blk"),
        P(None, "blk", None, "rhs", None, None),
        P("blk", None),
        P("blk", None),
        P(None, "blk", None),
    )
    return jax.shard_map(
        functools.partial(local, mesh.shape["blk"]),
        mesh=mesh, in_specs=in_specs, out_specs=P("blk", "rhs"), check_vma=False,
    )
```

```python
import functools

import jax
import jax.numpy as jnp
from jax import lax
from jax.experimental import pallas as pl
from jax.experimental.pallas import tpu as pltpu
from jax.sharding import PartitionSpec as P

LANES = 128
ROWS = 16
MESH = pl.DeviceIdType.MESH


def turn(values):
    half = values.shape[-1] // 2
    return jnp.concatenate([-values[:, half:], values[:, :half]], axis=1)


def levels_kernel(
    n, order, first_hbm, lf_hbm, rf_hbm, coef, flipped,
    head, tail, loose, rf, send, arr,
    load_sem, w_send, w_recv, a_send, a_recv,
):
    levels, _, _, depth, rank, _ = head.shape
    width = LANES + loose.shape[-1]
    blocks = coef.shape[0]
    points = rf.shape[1]
    per = blocks // n
    half = n // 2
    sources = n // 4
    me = lax.axis_index("blk")
    col = lax.axis_index("rhs")
    side = me // half
    place = lax.rem(me, half)

    def loads(l):
        return (
            pltpu.make_async_copy(
                lf_hbm.at[l, :, :, :, pl.ds(0, LANES)], head.at[l, col], load_sem.at[l, 0]
            ),
            pltpu.make_async_copy(
                lf_hbm.at[l, :, :, :, pl.ds(LANES, width - LANES)], loose.at[l], load_sem.at[l, 1]
            ),
        )

    load_coef = pltpu.make_async_copy(first_hbm, coef, load_sem.at[levels, 0])
    load_rows = pltpu.make_async_copy(rf_hbm, rf, load_sem.at[levels, 1])
    load_coef.start()
    for l in range(levels):
        for copy in loads(l):
            copy.start()
    load_rows.start()

    barrier = pltpu.get_barrier_semaphore()

    def greet(k, carry):
        peer = lax.rem(me + k, n)
        pl.semaphore_signal(barrier, inc=1, device_id=(peer, col), device_id_type=MESH)
        return carry

    lax.fori_loop(1, n, greet, 0)
    pl.semaphore_signal(barrier, inc=1, device_id=(me, 1 - col), device_id_type=MESH)

    def weight_copies(l, owner):
        return [
            pltpu.make_async_remote_copy(
                src_ref=ref.at[l, owner],
                dst_ref=ref.at[l, owner],
                send_sem=w_send.at[l, at],
                recv_sem=w_recv.at[l, at],
                device_id=(me, 1 - col),
                device_id_type=MESH,
            )
            for at, ref in enumerate((head, tail))
        ]

    def pack(l):
        def one(i, carry):
            tail[l, col, i] = jnp.concatenate([loose[l, 0, i], loose[l, 1, i]], axis=1)
            return carry

        lax.fori_loop(0, depth, one, 0, unroll=4)

    def block_copy(par, peer):
        return pltpu.make_async_remote_copy(
            src_ref=send.at[peer],
            dst_ref=arr.at[par, me],
            send_sem=a_send.at[peer],
            recv_sem=a_recv.at[par, me],
            device_id=(peer, col),
            device_id_type=MESH,
        )

    def arrival(par, source):
        return pltpu.make_async_remote_copy(
            src_ref=send.at[source],
            dst_ref=arr.at[par, source],
            send_sem=a_send.at[source],
            recv_sem=a_recv.at[par, source],
            device_id=(source, col),
            device_id_type=MESH,
        )

    def across(k):
        return (1 - side) * half + lax.rem(place + k, half)

    def beside(k):
        return side * half + lax.rem(place + k, half)

    blank = jnp.zeros((2 * LANES - width, LANES), jnp.bfloat16)

    load_coef.wait()
    pl.semaphore_wait(barrier, n)

    def level(l, carry):
        par = lax.rem(l, 2)

        def choose(peer):
            for q in range(per):
                send[peer, q] = coef[order[l, peer * per + q]]

        def hand_out(k, inner):
            choose(across(k))
            block_copy(par, across(k)).start()

            @pl.when(k > 0)
            def _():
                choose(beside(k))
                block_copy(par, beside(k)).start()

            return inner

        lax.fori_loop(0, half, hand_out, 0)
        choose(me)
        pltpu.make_async_copy(send.at[me], arr.at[par, me], a_recv.at[par, me]).start()

        @pl.when(l == 0)
        def _():
            for later in range(levels):
                for copy in loads(later):
                    copy.wait()
                pack(later)
                for copy in weight_copies(later, col):
                    copy.start()
            load_rows.wait()

            def flip(c, inner):
                base = pl.multiple_of(c * LANES, LANES)
                flipped[pl.ds(base, LANES), :] = rf[:, pl.ds(base, LANES)].T
                return inner

            lax.fori_loop(0, points // LANES, flip, 0, unroll=4)

        for copy in weight_copies(l, 1 - col):
            copy.wait_recv()

        def combine(k, inner):
            s = lax.rem(place + half - k, half)
            owner = s // sources
            at = lax.rem(s, sources) * per
            arrival(par, s).wait_recv()
            arrival(par, s + half).wait_recv()
            for q in range(per):
                i = at + q
                x = arr[par, s, q]
                y = arr[par, s + half, q]
                jx = turn(x)
                jy = turn(y)
                rest = tail[l, owner, i]
                upper = jnp.concatenate([head[l, owner, 0, i], rest], axis=1)
                lower = jnp.concatenate([head[l, owner, 1, i], rest], axis=1)
                cut = LANES - 2 * rank
                over = jnp.concatenate([x, jx, y, jy, blank], axis=0)
                under = jnp.concatenate([y, jy, x[:cut], blank, x[cut:], jx], axis=0)
                coef[s * per + q] = jnp.dot(
                    upper, over, preferred_element_type=jnp.float32
                ).astype(jnp.bfloat16)
                coef[(s + half) * per + q] = jnp.dot(
                    lower, under, preferred_element_type=jnp.float32
                ).astype(jnp.bfloat16)
            return inner

        lax.fori_loop(0, half, combine, 0)

        def sent(k, inner):
            block_copy(par, lax.rem(me + k, n)).wait_send()
            return inner

        lax.fori_loop(1, n, sent, 0)
        return carry

    lax.fori_loop(0, levels, level, 0)
    for l in range(levels):
        for copy in weight_copies(l, col):
            copy.wait_send()


def leaves_kernel(sizes, sig, cf, coef):
    blocks, rank, _ = coef.shape
    points = sig.shape[0]
    window = 2 * LANES
    lane = lax.broadcasted_iota(jnp.int32, (1, window), 1)

    def leaf(b, start):
        end = start + sizes[0, b]
        base = jnp.minimum(start // LANES * LANES, points - window)
        base = pl.multiple_of(base, LANES)
        inside = jnp.logical_and(lane >= start - base, lane < end - base)
        keep = jnp.where(inside, 1.0, 0.0).astype(jnp.bfloat16)
        weights = cf[:, pl.ds(base, window)] * keep
        sums = jnp.dot(weights, sig[pl.ds(base, window), :], preferred_element_type=jnp.float32)
        coef[b] = (sums[:rank] + turn(sums[rank:])).astype(jnp.bfloat16)
        return end

    lax.fori_loop(0, blocks, leaf, jnp.int32(0), unroll=8)


def rows_kernel(sizes, coef, flipped, out_hbm, out, sem):
    blocks, rank, _ = coef.shape
    points = out_hbm.shape[0]
    window = LANES + ROWS
    row = lax.broadcasted_iota(jnp.int32, (ROWS, LANES), 0)

    def leaf(b, start):
        base = pl.multiple_of(start // ROWS * ROWS, ROWS)
        values = coef[b]
        pair = jnp.concatenate([values, turn(values)], axis=0)
        sums = jnp.dot(flipped[pl.ds(base, window), :], pair, preferred_element_type=jnp.float32)
        before = out[pl.ds(base, ROWS), :].astype(jnp.float32)
        top = jnp.where(row < start - base, before, sums[:ROWS])
        out[pl.ds(base, ROWS), :] = top.astype(jnp.bfloat16)
        out[pl.ds(base + ROWS, LANES), :] = sums[ROWS:].astype(jnp.bfloat16)
        return start + sizes[0, b]

    lax.fori_loop(0, blocks, leaf, jnp.int32(0), unroll=8)
    copy = pltpu.make_async_copy(out.at[pl.ds(0, points)], out_hbm, sem)
    copy.start()
    copy.wait()


def local(
    n, signal, col_factor, row_factor, level_factor, col_leaf_sizes, row_leaf_sizes, level_order
):
    levels, _, halves, depth, rank, width = level_factor.shape
    blocks = col_leaf_sizes.shape[1]
    points, columns = signal.shape
    bf16 = jnp.bfloat16
    smem = pl.BlockSpec(memory_space=pltpu.SMEM)
    vmem = pl.BlockSpec(memory_space=pltpu.VMEM)
    anywhere = pl.BlockSpec(memory_space=pl.ANY)
    first = pl.pallas_call(
        leaves_kernel,
        out_shape=jax.ShapeDtypeStruct((blocks, row_factor.shape[0] // 2, columns), bf16),
        in_specs=[smem, vmem, vmem],
        out_specs=vmem,
        compiler_params=pltpu.CompilerParams(vmem_limit_bytes=32 << 20),
        name="leaves",
    )(col_leaf_sizes, signal, col_factor)
    factors = level_factor.reshape(levels, halves, depth, rank, width)
    coefficients, flipped = pl.pallas_call(
        functools.partial(levels_kernel, n),
        out_shape=(
            jax.ShapeDtypeStruct((blocks, rank, columns), bf16),
            jax.ShapeDtypeStruct((points + LANES + ROWS, 2 * rank), bf16),
        ),
        in_specs=[smem, anywhere, anywhere, anywhere],
        out_specs=(vmem, vmem),
        scratch_shapes=[
            pltpu.VMEM((levels, 2, halves, depth, rank, LANES), bf16),
            pltpu.VMEM((levels, 2, depth, rank, LANES), bf16),
            pltpu.VMEM((levels, halves, depth, rank, width - LANES), bf16),
            pltpu.VMEM((2 * rank, points), bf16),
            pltpu.VMEM((n, blocks // n, rank, columns), bf16),
            pltpu.VMEM((2, n, blocks // n, rank, columns), bf16),
            pltpu.SemaphoreType.DMA((levels + 1, 2)),
            pltpu.SemaphoreType.DMA((levels, 2)),
            pltpu.SemaphoreType.DMA((levels, 2)),
            pltpu.SemaphoreType.DMA((n,)),
            pltpu.SemaphoreType.DMA((2, n)),
        ],
        compiler_params=pltpu.CompilerParams(
            collective_id=0, has_side_effects=True, vmem_limit_bytes=48 << 20
        ),
        name="levels",
    )(level_order.reshape(levels, blocks), first, factors, row_factor)
    return pl.pallas_call(
        rows_kernel,
        out_shape=jax.ShapeDtypeStruct((points, columns), bf16),
        in_specs=[smem, vmem, vmem],
        out_specs=anywhere,
        scratch_shapes=[
            pltpu.VMEM((points + LANES + ROWS, columns), bf16),
            pltpu.SemaphoreType.DMA(()),
        ],
        compiler_params=pltpu.CompilerParams(vmem_limit_bytes=40 << 20),
        name="rows",
    )(row_leaf_sizes, coefficients, flipped)


def solution(mesh):
    in_specs = (
        P("blk", "rhs"),
        P(None, "blk"),
        P(None, "blk"),
        P(None, "blk", None, "rhs", None, None),
        P("blk", None),
        P("blk", None),
        P(None, "blk", None),
    )
    return jax.shard_map(
        functools.partial(local, mesh.shape["blk"]),
        mesh=mesh, in_specs=in_specs, out_specs=P("blk", "rhs"), check_vma=False,
    )
```
